32 devices in a mesh: row: 8 (over y, x, core), col: 4 (over z).
Axes of the slice: x: 2, y: 2, z: 4, core: 2. Of those that a mesh axis runs over, the one named last changes fastest.
Arguments:
- species: float32 [4, 64, 32, 256], P(None, None, 'row', 'col'), may hold values from -6 to 6
- symbol_x: float32 [64], replicated, may hold values from 0.3 to 3
- symbol_y: float32 [32], replicated, may hold values from 0.3 to 3
- symbol_z: float32 [256], replicated, may hold values from 0.3 to 3
Outputs:
- coefficients: float32 [4, 64, 32, 256], P(None, 'row', 'col')
The draws below stay inside these ranges and needn't reach their ends.
All inputs are finite; a program needn't handle non-finite values.
Results may differ from the reference program's by a relative error of at most 0.00007.
Values sent between devices are 32-bit elements; how exact they have to be, the bound alone decides.
A program may use at most 64 MiB of HBM per device.

```python
import jax
import jax.numpy as jnp
from jax import lax

GRID_X = 64
GRID_Y = 32
GRID_Z = 256
FIELDS = 4


def levels(key, extent, split, smallest, largest):
    def one(axis_at, parts):
        draws = jax.random.uniform(jax.random.fold_in(jax.random.fold_in(key, 6), axis_at), (parts,), jnp.float32, smallest / len(split), largest / len(split))
        return jnp.repeat(jnp.exp(draws), extent[axis_at] // parts).reshape((-1,) + (1,) * (len(extent) - axis_at - 1))

    factor_of = one(*split[0])
    for cut in split[1:]:
        factor_of = factor_of * one(*cut)
    return factor_of


def bell_draw(key, shape, width, bound, pieces=(), kind=jnp.bfloat16):
    array = width * jax.random.normal(key, shape, jnp.float32)
    if pieces:
        array = array * levels(key, shape, pieces, -0.22, 0.18)
    return jnp.clip(array, -bound, bound).astype(kind)


def setup_inputs(seed: int = 0) -> dict:
    key_of = jax.random.split(jax.random.key(seed), 5)
    species = bell_draw(key_of[0], (FIELDS, GRID_X, GRID_Y, GRID_Z), 1.0, 6.0, ((2, 8), (3, 4)), jnp.float32)
    symbol_x = jnp.clip(jax.random.uniform(key_of[1], (GRID_X,), jnp.float32, 0.3, 3.0), 0.3, 3.0)
    symbol_y = jnp.clip(jax.random.uniform(key_of[2], (GRID_Y,), jnp.float32, 0.3, 3.0), 0.3, 3.0)
    symbol_z = jnp.clip(jax.random.uniform(key_of[3], (GRID_Z,), jnp.float32, 0.3, 3.0), 0.3, 3.0)
    return dict(species=species, symbol_x=symbol_x, symbol_y=symbol_y, symbol_z=symbol_z)


def transform_table(count):
    rank = jnp.arange(count)
    angle = (jnp.pi / (count + 1)) * (((rank[:, None] + 1) * (rank[None, :] + 1)) % (2 * count + 2)).astype(jnp.float32)
    return jnp.sin(angle) * (2.0 / (count + 1)) ** 0.5


def transform_dim(values, dim):
    moved = jnp.tensordot(values, transform_table(values.shape[dim]), axes=([dim], [0]), precision=lax.Precision.HIGHEST)
    return jnp.moveaxis(moved, -1, dim)


def reference(species, symbol_x, symbol_y, symbol_z):
    coefficients = species
    coefficients = transform_dim(coefficients, 1)
    coefficients = transform_dim(coefficients, 2)
    coefficients = transform_dim(coefficients, 3)
    symbol = symbol_x[:, None, None] + symbol_y[None, :, None] + symbol_z[None, None, :]
    coefficients = coefficients / symbol
    return coefficients
```

```python
import functools

import jax
import jax.numpy as jnp
import ml_dtypes
import numpy as np
from jax import lax
from jax.experimental import pallas as pl
from jax.experimental.pallas import tpu as pltpu
from jax.sharding import PartitionSpec as P

MESH = pl.DeviceIdType.MESH
LANES = 128
SUBLANES = 8


def table(count):
    rank = np.arange(count, dtype=np.int64) + 1
    angle = np.pi / (count + 1) * ((rank[:, None] * rank[None, :]) % (2 * count + 2))
    return (np.sin(angle) * (2.0 / (count + 1)) ** 0.5).astype(np.float32)


def halves(values):
    high = values.astype(ml_dtypes.bfloat16)
    low = (values - high.astype(np.float32)).astype(ml_dtypes.bfloat16)
    return np.stack([high, low])


def split(values):
    high = values.astype(jnp.bfloat16)
    low = (values - high.astype(jnp.float32)).astype(jnp.bfloat16)
    return high, low


def side_by_side(values):
    return jnp.concatenate(split(values), axis=-1)


def dot(a, b):
    return jnp.dot(a, b, preferred_element_type=jnp.float32)


def left_dot(both, data):
    count, width = both.shape[0] // 2, data.shape[-1] // 2
    terms = dot(both, data)
    sides = terms[:, :width] + terms[:, width:]
    return sides[:count] + sides[count:]


def partner(me, step, count):
    if count & (count - 1):
        return lax.rem(me + step, count)
    to, bit = me, 1
    while bit < count:
        if step & bit:
            to = to + bit * (1 - 2 * lax.rem(me // bit, 2))
        bit *= 2
    return to


def chunk_list(cuts, groups):
    if cuts == 4 and groups == 2:
        return [(0, 0, 1), (0, 1, 1), (0, 2, 2), (1, 0, 2), (1, 2, 2)]
    return [(g, q, 1) for g in range(groups) for q in range(cuts)]


def batch_list(count):
    return [[0, 1], [2], [3], [4]]


ORDERS = (
    (3, 2, 1), (0, 3, 2), (3, 0, 1), (0, 1, 2),
    (3, 2, 1), (0, 3, 2), (3, 0, 1), (0, 1, 2),
    (3, 2, 1), (0, 3, 2), (3, 0, 1), (0, 1, 2),
    (3, 2, 1), (0, 3, 2), (3, 0, 1), (0, 1, 2),
)
EARLY = (
    (1, 0, 0), (1, 1, 0), (1, 1, 0), (1, 0, 0),
    (1, 0, 0), (1, 1, 0), (1, 1, 0), (0, 0, 0),
    (1, 0, 0), (1, 1, 0), (1, 1, 0), (1, 0, 0),
    (1, 0, 0), (1, 1, 0), (1, 1, 0), (1, 0, 0),
)


def pick(at, values):
    return sum(value * jnp.maximum(0, 1 - abs(at - i)) for i, value in enumerate(values) if value)


def passes(row, col, count):
    if count != 4:
        return [(partner(col, count - 1 - slot, count), 1 - min(slot, 1)) for slot in range(count - 1)]
    small = jnp.minimum(row, 2)
    at = count * (small + lax.div(small, 2) * lax.rem(row, 2)) + col
    return [(pick(at, [o[s] for o in ORDERS]), pick(at, [e[s] for e in EARLY])) for s in range(count - 1)]


def kernel(
    dims,
    species, symbol_x, symbol_y, symbol_z, table_x, table_y, table_z,
    out,
    space, mx, my, mz, sx, sy, sz, send_a, recv_a, send_b, recv_b, inverse,
    a_send, a_recv, b_send, b_recv, ready,
):
    fields, pack, rows, cols, cuts, xc, yb, zl = dims
    groups = fields // pack
    row, col = lax.axis_index("row"), lax.axis_index("col")
    chunks = chunk_list(cuts, groups)

    row_steps = list(range(rows - 1, 0, -1))
    col_steps = list(range(cols - 1, 0, -1))
    barrier = pltpu.get_barrier_semaphore()
    odd = lax.rem(row, 2)
    twin = row + 1 - 2 * odd

    def first_part(load_sem):
        pieces = [(species.at[f], space.at[f]) for f in range(fields)]
        pieces += [(table_x.at[q], mx.at[q]) for q in range(cuts)]
        pieces += [(symbol_x, sx), (symbol_y, sy), (symbol_z, sz), (table_y, my), (table_z, mz)]
        loads = [pltpu.make_async_copy(src, dst, load_sem.at[i]) for i, (src, dst) in enumerate(pieces)]
        urgent = list(range(pack)) + [fields]
        for i in urgent:
            loads[i].start()
        for pair in range(rows // 2):
            @pl.when(row != 2 * pair + 1)
            def _():
                pl.semaphore_signal(barrier, inc=1, device_id={"row": 2 * pair + 1}, device_id_type=MESH)
        for step in col_steps:
            to = {"row": row - odd, "col": partner(col, step, cols)}
            pl.semaphore_signal(barrier, inc=1, device_id=to, device_id_type=MESH)

        @pl.when(odd == 1)
        def _():
            pl.semaphore_signal(barrier, inc=1, device_id={"row": twin}, device_id_type=MESH)

        for i in range(fields + cuts):
            if i not in urgent:
                loads[i].start()

        for i, (g, q, n) in enumerate(chunks):
            if q == 0:
                for k in range(pack):
                    loads[g * pack + k].wait()
                data = side_by_side(jnp.concatenate([space[g * pack + k] for k in range(pack)], axis=-1))
            if g == 0:
                for p in range(q, q + n):
                    loads[fields + p].wait()
            for p in range(q, q + n):
                send_a[g, :, p] = left_dot(mx[p], data).reshape(rows, -1, LANES)
            if i == 0:

                @pl.when(odd == 1)
                def _():
                    pl.semaphore_wait(barrier, len(row_steps))
                    pl.semaphore_signal(ready, inc=1, device_id={"row": twin}, device_id_type=MESH)

                @pl.when(odd == 0)
                def _():
                    pl.semaphore_wait(ready, 1)

            for even_step, odd_step in zip(row_steps[1::2] + row_steps[::2], row_steps[::2] + row_steps[1::2]):
                to = partner(row, even_step, rows)
                to = to + (partner(row, odd_step, rows) - to) * odd
                pltpu.make_async_remote_copy(
                    src_ref=send_a.at[g, to, pl.ds(q, n)], dst_ref=recv_a.at[g, row, pl.ds(q, n)],
                    send_sem=a_send, recv_sem=a_recv.at[i],
                    device_id={"row": to}, device_id_type=MESH,
                ).start()
            recv_a[g, row, pl.ds(q, n)] = send_a[g, row, pl.ds(q, n)]
            if i == 0:
                for load in loads[fields + cuts:]:
                    load.start()

        for load in loads[fields + cuts:]:
            load.wait()
        part_y = jnp.zeros((yb, 1), jnp.float32)
        at = lax.broadcasted_iota(jnp.int32, (yb, 1), 0)
        for j in range(yb):
            part_y = jnp.where(at == j, sy[col * yb + j], part_y)
        for i in range(cuts * xc):
            inverse[i] = 1.0 / ((sx[row * (cuts * xc) + i] + part_y) + sz[...])

    pl.run_scoped(first_part, pltpu.SemaphoreType.DMA((fields + cuts + 5,)))

    @pl.when(odd == 0)
    def _():
        pl.semaphore_wait(barrier, 2 * len(col_steps) + 1)
        pl.semaphore_signal(ready, inc=1, device_id={"row": twin}, device_id_type=MESH)

    @pl.when(odd == 1)
    def _():
        pl.semaphore_wait(ready, 1)

    batches = batch_list(len(chunks))
    hops = passes(row, col, cols)

    def batch_of(i):
        return [i in batch for batch in batches].index(True)

    def pass_on(i, slot):
        g, q, n = chunks[i]
        to = hops[slot][0]
        pltpu.make_async_remote_copy(
            src_ref=send_b.at[g, to, pl.ds(q, n)], dst_ref=recv_b.at[g, col, pl.ds(q, n)],
            send_sem=b_send, recv_sem=b_recv.at[batch_of(i)],
            device_id={"col": to}, device_id_type=MESH,
        ).start()

    for i, (g, q, n) in enumerate(chunks):
        arrived = recv_a.at[g, pl.ds(0, rows - 1), pl.ds(q, n)]
        pltpu.make_async_copy(arrived, arrived, a_recv.at[i]).wait()
        for p in range(q, q + n):
            lines = recv_a[g, :, p].reshape(-1, LANES)
            send_b[g, :, p] = left_dot(my[...], side_by_side(lines)).reshape(cols, -1, LANES)
        for slot in range(cols - 1):
            pl.when(hops[slot][1] == 1)(functools.partial(pass_on, i, slot))
        recv_b[g, col, pl.ds(q, n)] = send_b[g, col, pl.ds(q, n)]
    for slot in range(cols - 1):
        for i in range(len(chunks)):
            pl.when(hops[slot][1] == 0)(functools.partial(pass_on, i, slot))

    height = xc * yb
    for batch in batches:
        lines = []
        g, q, n = chunks[batch[0]]
        arrived = recv_b.at[g, pl.ds(0, cols - 1), pl.ds(q, sum(chunks[i][2] for i in batch))]
        pltpu.make_async_copy(arrived, arrived, b_recv.at[batch_of(batch[0])]).wait()
        for i in batch:
            g, q, n = chunks[i]
            for p in range(q, q + n):
                blocks = [recv_b[g, c, p] for c in range(cols)]
                for k in range(pack):
                    lines.append(jnp.concatenate([b[:, k * zl:(k + 1) * zl] for b in blocks], axis=-1))
        high, low = split(jnp.concatenate(lines, axis=0))
        most = dot(jnp.concatenate([high, low], axis=0), mz[0])
        count = high.shape[0]
        result = most[:count] + most[count:] + dot(high, mz[1])
        at_line = 0
        for i in batch:
            g, q, n = chunks[i]
            for p in range(q, q + n):
                factor = inverse[p * xc:(p + 1) * xc].reshape(height, -1)
                for k in range(pack):
                    out[g * pack + k, pl.ds(p * height, height)] = result[at_line:at_line + height] * factor
                    at_line += height

    sent = send_a.at[:, pl.ds(0, rows - 1)]
    pltpu.make_async_copy(sent, sent, a_send).wait()
    sent = send_b.at[:, pl.ds(0, cols - 1)]
    pltpu.make_async_copy(sent, sent, b_send).wait()


def on_device(rows, cols, species, symbol_x, symbol_y, symbol_z):
    fields, x, yl, zl = species.shape
    y, z = symbol_y.shape[0], symbol_z.shape[0]
    xb, yb = x // rows, y // cols
    pack = LANES // zl
    groups = fields // pack
    xc = max(1, SUBLANES // yl)
    cuts = xb // xc

    hx = table(x)
    eye = np.eye(yl, dtype=np.float32)
    full_x = np.einsum("rqia,yb->qriyab", hx.T.reshape(rows, cuts, xc, x), eye).reshape(cuts, rows * xc * yl, x * yl)
    hy = table(y).T.reshape(cols, yb, rows, yl)
    full_y = np.einsum("cmry,ij->cimrjy", hy, np.eye(xc, dtype=np.float32)).reshape(cols * xc * yb, rows * xc * yl)
    tables = [
        np.concatenate(list(halves(full_x)), axis=1), np.concatenate(list(halves(full_y)), axis=0), halves(table(z))
    ]

    any_space = pl.BlockSpec(memory_space=pltpu.MemorySpace.HBM)
    chunks = len(chunk_list(cuts, groups))
    a_shape = (groups, rows, cuts, xc * yl, LANES)
    b_shape = (groups, cols, cuts, xc * yb, LANES)
    dma = pltpu.SemaphoreType.DMA
    out = pl.pallas_call(
        functools.partial(kernel, (fields, pack, rows, cols, cuts, xc, yb, zl)),
        out_shape=pltpu.MemorySpace.VMEM((fields, xb * yb, z), jnp.float32),
        in_specs=[any_space] * 7,
        out_specs=pl.BlockSpec(memory_space=pltpu.MemorySpace.VMEM),
        scratch_shapes=[
            pltpu.VMEM((fields, x * yl, zl), jnp.float32),
            pltpu.VMEM(tables[0].shape, jnp.bfloat16),
            pltpu.VMEM(tables[1].shape, jnp.bfloat16),
            pltpu.VMEM(tables[2].shape, jnp.bfloat16),
            pltpu.SMEM((x,), jnp.float32),
            pltpu.SMEM((y,), jnp.float32),
            pltpu.VMEM((1, z), jnp.float32),
            pltpu.VMEM(a_shape, jnp.float32),
            pltpu.VMEM(a_shape, jnp.float32),
            pltpu.VMEM(b_shape, jnp.float32),
            pltpu.VMEM(b_shape, jnp.float32),
            pltpu.VMEM((xb, yb, z), jnp.float32),
            dma,
            dma((chunks,)),
            dma,
            dma((len(batch_list(chunks)),)),
            pltpu.SemaphoreType.REGULAR,
        ],
        compiler_params=pltpu.CompilerParams(
            collective_id=0, has_side_effects=True, vmem_limit_bytes=60 * 1024 * 1024
        ),
    )(
        species.reshape(fields, x * yl, zl), symbol_x, symbol_y, symbol_z.reshape(1, z),
        *[jnp.asarray(t) for t in tables],
    )
    return out.reshape(fields, xb, yb, z)


def solution(mesh):
    placed = (P(None, None, "row", "col"), P(), P(), P())
    return jax.shard_map(
        functools.partial(on_device, mesh.shape["row"], mesh.shape["col"]),
        mesh=mesh,
        in_specs=placed,
        out_specs=P(None, "row", "col", None),
        check_vma=False,
    )
```

```python
import functools

import jax
import jax.numpy as jnp
import ml_dtypes
import numpy as np
from jax import lax
from jax.experimental import pallas as pl
from jax.experimental.pallas import tpu as pltpu
from jax.sharding import PartitionSpec as P

MESH = pl.DeviceIdType.MESH
LANES = 128
SUBLANES = 8


def table(count):
    rank = np.arange(count, dtype=np.int64) + 1
    angle = np.pi / (count + 1) * ((rank[:, None] * rank[None, :]) % (2 * count + 2))
    return (np.sin(angle) * (2.0 / (count + 1)) ** 0.5).astype(np.float32)


def halves(values):
    high = values.astype(ml_dtypes.bfloat16)
    low = (values - high.astype(np.float32)).astype(ml_dtypes.bfloat16)
    return np.stack([high, low])


def split(values):
    high = values.astype(jnp.bfloat16)
    low = (values - high.astype(jnp.float32)).astype(jnp.bfloat16)
    return high, low


def side_by_side(values):
    return jnp.concatenate(split(values), axis=-1)


def dot(a, b):
    return jnp.dot(a, b, preferred_element_type=jnp.float32)


def left_dot(both, data):
    count, width = both.shape[0] // 2, data.shape[-1] // 2
    terms = dot(both, data)
    sides = terms[:, :width] + terms[:, width:]
    return sides[:count] + sides[count:]


def partner(me, step, count):
    if count & (count - 1):
        return lax.rem(me + step, count)
    to, bit = me, 1
    while bit < count:
        if step & bit:
            to = to + bit * (1 - 2 * lax.rem(me // bit, 2))
        bit *= 2
    return to


def chunk_list(cuts, groups):
    if cuts == 4 and groups == 2:
        return [(0, 0, 1), (0, 1, 1), (0, 2, 2), (1, 0, 2), (1, 2, 2)]
    return [(g, q, 1) for g in range(groups) for q in range(cuts)]


def batch_list(count):
    return [[0, 1], [2], [3], [4]] if count == 5 else [[i] for i in range(count)]


ORDERS = (
    (3, 2, 1), (0, 3, 2), (3, 0, 1), (0, 1, 2),
    (3, 2, 1), (0, 3, 2), (3, 0, 1), (0, 1, 2),
    (3, 2, 1), (0, 3, 2), (3, 0, 1), (0, 1, 2),
    (3, 2, 1), (0, 3, 2), (3, 0, 1), (0, 2, 1),
)
EARLY = (
    (1, 0, 0), (1, 1, 0), (1, 1, 0), (1, 0, 0),
    (1, 0, 0), (1, 1, 0), (1, 1, 1), (0, 0, 0),
    (1, 0, 0), (1, 1, 0), (1, 1, 0), (1, 0, 0),
    (1, 0, 0), (1, 1, 0), (1, 1, 1), (1, 0, 0),
)


def pick(at, values):
    return sum(value * jnp.maximum(0, 1 - abs(at - i)) for i, value in enumerate(values) if value)


def passes(row, col, count):
    if count != 4:
        return [(partner(col, count - 1 - slot, count), 1 - min(slot, 1)) for slot in range(count - 1)]
    small = jnp.minimum(row, 2)
    at = count * (small + lax.div(small, 2) * lax.rem(row, 2)) + col
    return [(pick(at, [o[s] for o in ORDERS]), pick(at, [e[s] for e in EARLY])) for s in range(count - 1)]


def kernel(
    dims,
    species, symbol_x, symbol_y, symbol_z, table_x, table_y, table_z,
    out,
    space, mx, my, mz, sx, sy, sz, send_a, recv_a, send_b, recv_b, inverse,
    a_send, a_recv, b_send, b_recv, ready,
):
    fields, pack, rows, cols, cuts, xc, yb, zl = dims
    groups = fields // pack
    row, col = lax.axis_index("row"), lax.axis_index("col")
    chunks = chunk_list(cuts, groups)

    row_steps = list(range(rows - 1, 0, -1))
    col_steps = list(range(cols - 1, 0, -1))
    barrier = pltpu.get_barrier_semaphore()
    odd = lax.rem(row, 2)
    twin = row + 1 - 2 * odd

    def first_part(load_sem):
        pieces = [(species.at[f], space.at[f]) for f in range(fields)]
        pieces += [(table_x.at[q], mx.at[q]) for q in range(cuts)]
        pieces += [(symbol_x, sx), (symbol_y, sy), (symbol_z, sz), (table_y, my), (table_z, mz)]
        loads = [pltpu.make_async_copy(src, dst, load_sem.at[i]) for i, (src, dst) in enumerate(pieces)]
        urgent = list(range(pack)) + [fields]
        for i in urgent:
            loads[i].start()
        for pair in range(rows // 2):
            @pl.when(row != 2 * pair + 1)
            def _():
                pl.semaphore_signal(barrier, inc=1, device_id={"row": 2 * pair + 1}, device_id_type=MESH)
        for step in col_steps:
            to = {"row": row - odd, "col": partner(col, step, cols)}
            pl.semaphore_signal(barrier, inc=1, device_id=to, device_id_type=MESH)

        @pl.when(odd == 1)
        def _():
            pl.semaphore_signal(barrier, inc=1, device_id={"row": twin}, device_id_type=MESH)

        for i in range(fields + cuts):
            if i not in urgent:
                loads[i].start()

        for i, (g, q, n) in enumerate(chunks):
            if q == 0:
                for k in range(pack):
                    loads[g * pack + k].wait()
                data = side_by_side(jnp.concatenate([space[g * pack + k] for k in range(pack)], axis=-1))
            if g == 0:
                for p in range(q, q + n):
                    loads[fields + p].wait()
            for p in range(q, q + n):
                send_a[g, :, p] = left_dot(mx[p], data).reshape(rows, -1, LANES)
            if i == 0:

                @pl.when(odd == 1)
                def _():
                    pl.semaphore_wait(barrier, len(row_steps))
                    pl.semaphore_signal(ready, inc=1, device_id={"row": twin}, device_id_type=MESH)

                @pl.when(odd == 0)
                def _():
                    pl.semaphore_wait(ready, 1)

            for even_step, odd_step in zip(row_steps[1::2] + row_steps[::2], row_steps[::2] + row_steps[1::2]):
                to = partner(row, even_step, rows)
                to = to + (partner(row, odd_step, rows) - to) * odd
                pltpu.make_async_remote_copy(
                    src_ref=send_a.at[g, to, pl.ds(q, n)], dst_ref=recv_a.at[g, row, pl.ds(q, n)],
                    send_sem=a_send, recv_sem=a_recv.at[i],
                    device_id={"row": to}, device_id_type=MESH,
                ).start()
            recv_a[g, row, pl.ds(q, n)] = send_a[g, row, pl.ds(q, n)]
            if i == 0:
                for load in loads[fields + cuts:]:
                    load.start()

        for load in loads[fields + cuts:]:
            load.wait()
        part_y = jnp.zeros((yb, 1), jnp.float32)
        at = lax.broadcasted_iota(jnp.int32, (yb, 1), 0)
        for j in range(yb):
            part_y = jnp.where(at == j, sy[col * yb + j], part_y)
        for i in range(cuts * xc):
            inverse[i] = 1.0 / ((sx[row * (cuts * xc) + i] + part_y) + sz[...])

    pl.run_scoped(first_part, pltpu.SemaphoreType.DMA((fields + cuts + 5,)))

    @pl.when(odd == 0)
    def _():
        pl.semaphore_wait(barrier, 2 * len(col_steps) + 1)
        pl.semaphore_signal(ready, inc=1, device_id={"row": twin}, device_id_type=MESH)

    @pl.when(odd == 1)
    def _():
        pl.semaphore_wait(ready, 1)

    batches = batch_list(len(chunks))
    hops = passes(row, col, cols)

    def batch_of(i):
        return [i in batch for batch in batches].index(True)

    def pass_on(i, slot):
        g, q, n = chunks[i]
        to = hops[slot][0]
        pltpu.make_async_remote_copy(
            src_ref=send_b.at[g, to, pl.ds(q, n)], dst_ref=recv_b.at[g, col, pl.ds(q, n)],
            send_sem=b_send, recv_sem=b_recv.at[batch_of(i)],
            device_id={"col": to}, device_id_type=MESH,
        ).start()

    for i, (g, q, n) in enumerate(chunks):
        arrived = recv_a.at[g, pl.ds(0, rows - 1), pl.ds(q, n)]
        pltpu.make_async_copy(arrived, arrived, a_recv.at[i]).wait()
        for p in range(q, q + n):
            lines = recv_a[g, :, p].reshape(-1, LANES)
            send_b[g, :, p] = left_dot(my[...], side_by_side(lines)).reshape(cols, -1, LANES)
        for slot in range(cols - 1):
            pl.when(hops[slot][1] == 1)(functools.partial(pass_on, i, slot))
        recv_b[g, col, pl.ds(q, n)] = send_b[g, col, pl.ds(q, n)]
    for slot in range(cols - 1):
        for i in range(len(chunks)):
            pl.when(hops[slot][1] == 0)(functools.partial(pass_on, i, slot))

    height = xc * yb
    for batch in batches:
        lines = []
        g, q, n = chunks[batch[0]]
        arrived = recv_b.at[g, pl.ds(0, cols - 1), pl.ds(q, sum(chunks[i][2] for i in batch))]
        pltpu.make_async_copy(arrived, arrived, b_recv.at[batch_of(batch[0])]).wait()
        for i in batch:
            g, q, n = chunks[i]
            for p in range(q, q + n):
                blocks = [recv_b[g, c, p] for c in range(cols)]
                for k in range(pack):
                    lines.append(jnp.concatenate([b[:, k * zl:(k + 1) * zl] for b in blocks], axis=-1))
        high, low = split(jnp.concatenate(lines, axis=0))
        most = dot(jnp.concatenate([high, low], axis=0), mz[0])
        count = high.shape[0]
        result = most[:count] + most[count:] + dot(high, mz[1])
        at_line = 0
        for i in batch:
            g, q, n = chunks[i]
            for p in range(q, q + n):
                factor = inverse[p * xc:(p + 1) * xc].reshape(height, -1)
                for k in range(pack):
                    out[g * pack + k, pl.ds(p * height, height)] = result[at_line:at_line + height] * factor
                    at_line += height

    sent = send_a.at[:, pl.ds(0, rows - 1)]
    pltpu.make_async_copy(sent, sent, a_send).wait()
    sent = send_b.at[:, pl.ds(0, cols - 1)]
    pltpu.make_async_copy(sent, sent, b_send).wait()


def on_device(rows, cols, species, symbol_x, symbol_y, symbol_z):
    fields, x, yl, zl = species.shape
    y, z = symbol_y.shape[0], symbol_z.shape[0]
    xb, yb = x // rows, y // cols
    pack = LANES // zl
    groups = fields // pack
    xc = max(1, SUBLANES // yl)
    cuts = xb // xc

    hx = table(x)
    eye = np.eye(yl, dtype=np.float32)
    full_x = np.einsum("rqia,yb->qriyab", hx.T.reshape(rows, cuts, xc, x), eye).reshape(cuts, rows * xc * yl, x * yl)
    hy = table(y).T.reshape(cols, yb, rows, yl)
    full_y = np.einsum("cmry,ij->cimrjy", hy, np.eye(xc, dtype=np.float32)).reshape(cols * xc * yb, rows * xc * yl)
    tables = [
        np.concatenate(list(halves(full_x)), axis=1), np.concatenate(list(halves(full_y)), axis=0), halves(table(z))
    ]

    any_space = pl.BlockSpec(memory_space=pltpu.MemorySpace.HBM)
    chunks = len(chunk_list(cuts, groups))
    a_shape = (groups, rows, cuts, xc * yl, LANES)
    b_shape = (groups, cols, cuts, xc * yb, LANES)
    dma = pltpu.SemaphoreType.DMA
    out = pl.pallas_call(
        functools.partial(kernel, (fields, pack, rows, cols, cuts, xc, yb, zl)),
        out_shape=pltpu.MemorySpace.VMEM((fields, xb * yb, z), jnp.float32),
        in_specs=[any_space] * 7,
        out_specs=pl.BlockSpec(memory_space=pltpu.MemorySpace.VMEM),
        scratch_shapes=[
            pltpu.VMEM((fields, x * yl, zl), jnp.float32),
            pltpu.VMEM(tables[0].shape, jnp.bfloat16),
            pltpu.VMEM(tables[1].shape, jnp.bfloat16),
            pltpu.VMEM(tables[2].shape, jnp.bfloat16),
            pltpu.SMEM((x,), jnp.float32),
            pltpu.SMEM((y,), jnp.float32),
            pltpu.VMEM((1, z), jnp.float32),
            pltpu.VMEM(a_shape, jnp.float32),
            pltpu.VMEM(a_shape, jnp.float32),
            pltpu.VMEM(b_shape, jnp.float32),
            pltpu.VMEM(b_shape, jnp.float32),
            pltpu.VMEM((xb, yb, z), jnp.float32),
            dma,
            dma((chunks,)),
            dma,
            dma((len(batch_list(chunks)),)),
            pltpu.SemaphoreType.REGULAR,
        ],
        compiler_params=pltpu.CompilerParams(
            collective_id=0, has_side_effects=True, vmem_limit_bytes=60 * 1024 * 1024
        ),
    )(
        species.reshape(fields, x * yl, zl), symbol_x, symbol_y, symbol_z.reshape(1, z),
        *[jnp.asarray(t) for t in tables],
    )
    return out.reshape(fields, xb, yb, z)


def solution(mesh):
    placed = (P(None, None, "row", "col"), P(), P(), P())
    return jax.shard_map(
        functools.partial(on_device, mesh.shape["row"], mesh.shape["col"]),
        mesh=mesh,
        in_specs=placed,
        out_specs=P(None, "row", "col", None),
        check_vma=False,
    )
```

```python
import functools

import jax
import jax.numpy as jnp
import ml_dtypes
import numpy as np
from jax import lax
from jax.experimental import pallas as pl
from jax.experimental.pallas import tpu as pltpu
from jax.sharding import PartitionSpec as P

MESH = pl.DeviceIdType.MESH
LANES = 128
PIECES = 4
SUBLANES = 8


def table(count):
    rank = np.arange(count, dtype=np.int64) + 1
    angle = np.pi / (count + 1) * ((rank[:, None] * rank[None, :]) % (2 * count + 2))
    return (np.sin(angle) * (2.0 / (count + 1)) ** 0.5).astype(np.float32)


def halves(values):
    high = values.astype(ml_dtypes.bfloat16)
    low = (values - high.astype(np.float32)).astype(ml_dtypes.bfloat16)
    return np.stack([high, low])


def split(values):
    high = values.astype(jnp.bfloat16)
    low = (values - high.astype(jnp.float32)).astype(jnp.bfloat16)
    return high, low


def side_by_side(values):
    return jnp.concatenate(split(values), axis=-1)


def dot(a, b):
    return jnp.dot(a, b, preferred_element_type=jnp.float32)


def left_dot(both, data):
    count, width = both.shape[0] // 2, data.shape[-1] // 2
    terms = dot(both, data)
    sides = terms[:, :width] + terms[:, width:]
    return sides[:count] + sides[count:]


def partner(me, step, count):
    if count & (count - 1):
        return lax.rem(me + step, count)
    to, bit = me, 1
    while bit < count:
        if step & bit:
            to = to + bit * (1 - 2 * lax.rem(me // bit, 2))
        bit *= 2
    return to


def chunk_list(cuts, groups):
    if cuts == 4 and groups == 2:
        return [(0, 0, 1), (0, 1, 1), (0, 2, 2), (1, 0, 2), (1, 2, 2)]
    return [(g, q, 1) for g in range(groups) for q in range(cuts)]


def batch_list(count):
    return [[0, 1], [2], [3], [4]] if count == 5 else [[i] for i in range(count)]


ORDERS = (
    (3, 2, 1), (0, 3, 2), (3, 0, 1), (0, 1, 2),
    (3, 2, 1), (0, 3, 2), (3, 0, 1), (0, 1, 2),
    (3, 2, 1), (0, 3, 2), (3, 0, 1), (0, 1, 2),
    (3, 2, 1), (0, 3, 2), (3, 0, 1), (0, 2, 1),
)
EARLY = (
    (1, 0, 0), (1, 1, 0), (1, 1, 0), (1, 0, 0),
    (1, 0, 0), (1, 1, 0), (1, 1, 1), (0, 0, 0),
    (1, 0, 0), (1, 1, 0), (1, 1, 0), (1, 0, 0),
    (1, 0, 0), (1, 1, 0), (1, 1, 1), (1, 0, 0),
)


def pick(at, values):
    return sum(value * jnp.maximum(0, 1 - abs(at - i)) for i, value in enumerate(values) if value)


def passes(row, col, count):
    if count != 4:
        return [(partner(col, count - 1 - slot, count), 1 - min(slot, 1)) for slot in range(count - 1)]
    small = jnp.minimum(row, 2)
    at = count * (small + lax.div(small, 2) * lax.rem(row, 2)) + col
    return [(pick(at, [o[s] for o in ORDERS]), pick(at, [e[s] for e in EARLY])) for s in range(count - 1)]


def kernel(
    dims,
    species, symbol_x, symbol_y, symbol_z, table_x, table_y, table_z,
    out,
    space, mx, my, mz, sx, sy, sz, send_a, recv_a, send_b, recv_b, inverse,
    b_send, b_recv, ready,
):
    fields, pack, rows, cols, cuts, xc, yb, zl = dims
    groups = fields // pack
    row, col = lax.axis_index("row"), lax.axis_index("col")
    chunks = chunk_list(cuts, groups)

    row_steps = list(range(rows - 1, 0, -1))
    col_steps = list(range(cols - 1, 0, -1))
    barrier = pltpu.get_barrier_semaphore()
    odd = lax.rem(row, 2)
    twin = row + 1 - 2 * odd

    batches = batch_list(len(chunks))

    def batch_of(i):
        return [i in batch for batch in batches].index(True)

    def first_part(load_sem, a_send, a_recv):
        pieces = [(species.at[f], space.at[f]) for f in range(fields)]
        pieces += [(table_x.at[q], mx.at[q]) for q in range(cuts)]
        pieces += [(symbol_x, sx), (symbol_y, sy), (symbol_z, sz), (table_y, my), (table_z, mz)]
        loads = [
            None if i < pack else pltpu.make_async_copy(src, dst, load_sem.at[i])
            for i, (src, dst) in enumerate(pieces)
        ]
        loads[fields].start()
        height = space.shape[1] // PIECES
        for i in range(PIECES):
            for f in range(pack):
                part = pl.ds(i * height, height)
                pltpu.make_async_copy(species.at[f, part], space.at[f, part], load_sem.at[0]).start()
        for pair in range(rows // 2):
            @pl.when(row != 2 * pair + 1)
            def _():
                pl.semaphore_signal(barrier, inc=1, device_id={"row": 2 * pair + 1}, device_id_type=MESH)
        for step in col_steps:
            to = {"row": row - odd, "col": partner(col, step, cols)}
            pl.semaphore_signal(barrier, inc=1, device_id=to, device_id_type=MESH)

        @pl.when(odd == 1)
        def _():
            pl.semaphore_signal(barrier, inc=1, device_id={"row": twin}, device_id_type=MESH)

        for load in loads[fields + 1:fields + cuts]:
            load.start()

        for i, (g, q, n) in enumerate(chunks):
            if q == 0:
                if g == 0:
                    loads[fields].wait()
                    for load in loads[pack:fields]:
                        load.start()
                    group = space.at[pl.ds(0, pack)]
                    pltpu.make_async_copy(group, group, load_sem.at[0]).wait()
                else:
                    for k in range(pack):
                        loads[g * pack + k].wait()
                data = side_by_side(jnp.concatenate([space[g * pack + k] for k in range(pack)], axis=-1))
            if g == 0:
                for p in range(max(q, 1), q + n):
                    loads[fields + p].wait()
            for p in range(q, q + n):
                send_a[g, :, p] = left_dot(mx[p], data).reshape(rows, -1, LANES)
            if i == 0:

                @pl.when(odd == 1)
                def _():
                    pl.semaphore_wait(barrier, len(row_steps))
                    pl.semaphore_signal(ready, inc=1, device_id={"row": twin}, device_id_type=MESH)

                @pl.when(odd == 0)
                def _():
                    pl.semaphore_wait(ready, 1)

            for even_step, odd_step in zip(row_steps[1::2] + row_steps[::2], row_steps[::2] + row_steps[1::2]):
                to = partner(row, even_step, rows)
                to = to + (partner(row, odd_step, rows) - to) * odd
                pltpu.make_async_remote_copy(
                    src_ref=send_a.at[g, to, pl.ds(q, n)], dst_ref=recv_a.at[g, row, pl.ds(q, n)],
                    send_sem=a_send, recv_sem=a_recv.at[i],
                    device_id={"row": to}, device_id_type=MESH,
                ).start()
            recv_a[g, row, pl.ds(q, n)] = send_a[g, row, pl.ds(q, n)]
            if i == 0:
                for load in loads[fields + cuts:]:
                    load.start()

        for load in loads[fields + cuts:]:
            load.wait()
        part_y = jnp.zeros((yb, 1), jnp.float32)
        at = lax.broadcasted_iota(jnp.int32, (yb, 1), 0)
        for j in range(yb):
            part_y = jnp.where(at == j, sy[col * yb + j], part_y)
        for i in range(cuts * xc):
            inverse[i] = 1.0 / ((sx[row * (cuts * xc) + i] + part_y) + sz[...])


        @pl.when(odd == 0)
        def _():
            pl.semaphore_wait(barrier, 2 * len(col_steps) + 1)
            pl.semaphore_signal(ready, inc=1, device_id={"row": twin}, device_id_type=MESH)

        @pl.when(odd == 1)
        def _():
            pl.semaphore_wait(ready, 1)

        hops = passes(row, col, cols)

        def pass_on(i, slot):
            g, q, n = chunks[i]
            to = hops[slot][0]
            pltpu.make_async_remote_copy(
                src_ref=send_b.at[g, to, pl.ds(q, n)], dst_ref=recv_b.at[g, col, pl.ds(q, n)],
                send_sem=b_send, recv_sem=b_recv.at[batch_of(i)],
                device_id={"col": to}, device_id_type=MESH,
            ).start()

        for i, (g, q, n) in enumerate(chunks):
            arrived = recv_a.at[g, pl.ds(0, rows - 1), pl.ds(q, n)]
            pltpu.make_async_copy(arrived, arrived, a_recv.at[i]).wait()
            for p in range(q, q + n):
                lines = recv_a[g, :, p].reshape(-1, LANES)
                send_b[g, :, p] = left_dot(my[...], side_by_side(lines)).reshape(cols, -1, LANES)
            for slot in range(cols - 1):
                pl.when(hops[slot][1] == 1)(functools.partial(pass_on, i, slot))
            recv_b[g, col, pl.ds(q, n)] = send_b[g, col, pl.ds(q, n)]
        for slot in range(cols - 1):
            for i in range(len(chunks)):
                pl.when(hops[slot][1] == 0)(functools.partial(pass_on, i, slot))

        sent = send_a.at[:, pl.ds(0, rows - 1)]
        pltpu.make_async_copy(sent, sent, a_send).wait()

    dma = pltpu.SemaphoreType.DMA
    pl.run_scoped(first_part, dma((fields + cuts + 5,)), dma, dma((len(chunks),)))

    height = xc * yb
    for batch in batches:
        lines = []
        g, q, n = chunks[batch[0]]
        arrived = recv_b.at[g, pl.ds(0, cols - 1), pl.ds(q, sum(chunks[i][2] for i in batch))]
        pltpu.make_async_copy(arrived, arrived, b_recv.at[batch_of(batch[0])]).wait()
        for i in batch:
            g, q, n = chunks[i]
            for p in range(q, q + n):
                blocks = [recv_b[g, c, p] for c in range(cols)]
                for k in range(pack):
                    lines.append(jnp.concatenate([b[:, k * zl:(k + 1) * zl] for b in blocks], axis=-1))
        high, low = split(jnp.concatenate(lines, axis=0))
        most = dot(jnp.concatenate([high, low], axis=0), mz[0])
        count = high.shape[0]
        result = most[:count] + most[count:] + dot(high, mz[1])
        at_line = 0
        for i in batch:
            g, q, n = chunks[i]
            for p in range(q, q + n):
                factor = inverse[p * xc:(p + 1) * xc].reshape(height, -1)
                for k in range(pack):
                    out[g * pack + k, pl.ds(p * height, height)] = result[at_line:at_line + height] * factor
                    at_line += height

    sent = send_b.at[:, pl.ds(0, cols - 1)]
    pltpu.make_async_copy(sent, sent, b_send).wait()


def on_device(rows, cols, species, symbol_x, symbol_y, symbol_z):
    fields, x, yl, zl = species.shape
    y, z = symbol_y.shape[0], symbol_z.shape[0]
    xb, yb = x // rows, y // cols
    pack = LANES // zl
    groups = fields // pack
    xc = max(1, SUBLANES // yl)
    cuts = xb // xc

    hx = table(x)
    eye = np.eye(yl, dtype=np.float32)
    full_x = np.einsum("rqia,yb->qriyab", hx.T.reshape(rows, cuts, xc, x), eye).reshape(cuts, rows * xc * yl, x * yl)
    hy = table(y).T.reshape(cols, yb, rows, yl)
    full_y = np.einsum("cmry,ij->cimrjy", hy, np.eye(xc, dtype=np.float32)).reshape(cols * xc * yb, rows * xc * yl)
    tables = [
        np.concatenate(list(halves(full_x)), axis=1), np.concatenate(list(halves(full_y)), axis=0), halves(table(z))
    ]

    any_space = pl.BlockSpec(memory_space=pltpu.MemorySpace.HBM)
    chunks = len(chunk_list(cuts, groups))
    a_shape = (groups, rows, cuts, xc * yl, LANES)
    b_shape = (groups, cols, cuts, xc * yb, LANES)
    dma = pltpu.SemaphoreType.DMA
    out = pl.pallas_call(
        functools.partial(kernel, (fields, pack, rows, cols, cuts, xc, yb, zl)),
        out_shape=pltpu.MemorySpace.VMEM((fields, xb * yb, z), jnp.float32),
        in_specs=[any_space] * 7,
        out_specs=pl.BlockSpec(memory_space=pltpu.MemorySpace.VMEM),
        scratch_shapes=[
            pltpu.VMEM((fields, x * yl, zl), jnp.float32),
            pltpu.VMEM(tables[0].shape, jnp.bfloat16),
            pltpu.VMEM(tables[1].shape, jnp.bfloat16),
            pltpu.VMEM(tables[2].shape, jnp.bfloat16),
            pltpu.SMEM((x,), jnp.float32),
            pltpu.SMEM((y,), jnp.float32),
            pltpu.VMEM((1, z), jnp.float32),
            pltpu.VMEM(a_shape, jnp.float32),
            pltpu.VMEM(a_shape, jnp.float32),
            pltpu.VMEM(b_shape, jnp.float32),
            pltpu.VMEM(b_shape, jnp.float32),
            pltpu.VMEM((xb, yb, z), jnp.float32),
            dma,
            dma((len(batch_list(chunks)),)),
            pltpu.SemaphoreType.REGULAR,
        ],
        compiler_params=pltpu.CompilerParams(
            collective_id=0, has_side_effects=True, vmem_limit_bytes=60 * 1024 * 1024
        ),
    )(
        species.reshape(fields, x * yl, zl), symbol_x, symbol_y, symbol_z.reshape(1, z),
        *[jnp.asarray(t) for t in tables],
    )
    return out.reshape(fields, xb, yb, z)


def solution(mesh):
    placed = (P(None, None, "row", "col"), P(), P(), P())
    return jax.shard_map(
        functools.partial(on_device, mesh.shape["row"], mesh.shape["col"]),
        mesh=mesh,
        in_specs=placed,
        out_specs=P(None, "row", "col", None),
        check_vma=False,
    )
```

```python
import functools

import jax
import jax.numpy as jnp
import ml_dtypes
import numpy as np
from jax import lax
from jax.experimental import pallas as pl
from jax.experimental.pallas import tpu as pltpu
from jax.sharding import PartitionSpec as P

MESH = pl.DeviceIdType.MESH
LANES = 128
PIECES = 8
SUBLANES = 8


def table(count):
    rank = np.arange(count, dtype=np.int64) + 1
    angle = np.pi / (count + 1) * ((rank[:, None] * rank[None, :]) % (2 * count + 2))
    return (np.sin(angle) * (2.0 / (count + 1)) ** 0.5).astype(np.float32)


def halves(values):
    high = values.astype(ml_dtypes.bfloat16)
    low = (values - high.astype(np.float32)).astype(ml_dtypes.bfloat16)
    return np.stack([high, low])


def split(values):
    high = values.astype(jnp.bfloat16)
    low = (values - high.astype(jnp.float32)).astype(jnp.bfloat16)
    return high, low


def side_by_side(values):
    return jnp.concatenate(split(values), axis=-1)


def dot(a, b):
    return jnp.dot(a, b, preferred_element_type=jnp.float32)


def left_dot(both, data):
    count, width = both.shape[0] // 2, data.shape[-1] // 2
    terms = dot(both, data)
    sides = terms[:, :width] + terms[:, width:]
    return sides[:count] + sides[count:]


def partner(me, step, count):
    if count & (count - 1):
        return lax.rem(me + step, count)
    to, bit = me, 1
    while bit < count:
        if step & bit:
            to = to + bit * (1 - 2 * lax.rem(me // bit, 2))
        bit *= 2
    return to


def chunk_list(cuts, groups):
    if cuts == 4 and groups == 2:
        return [(0, 0, 1), (0, 1, 1), (0, 2, 2), (1, 0, 2), (1, 2, 2)]
    return [(g, q, 1) for g in range(groups) for q in range(cuts)]


def batch_list(count):
    return [[0, 1, 2], [3], [4]] if count == 5 else [[i] for i in range(count)]


ORDERS = (
    (3, 2, 1), (0, 3, 2), (3, 0, 1), (0, 1, 2),
    (3, 2, 1), (0, 3, 2), (3, 0, 1), (0, 1, 2),
    (3, 2, 1), (0, 3, 2), (3, 0, 1), (0, 1, 2),
    (3, 2, 1), (0, 3, 2), (3, 0, 1), (0, 2, 1),
)
EARLY = (
    (1, 0, 0), (1, 1, 0), (1, 1, 0), (1, 0, 0),
    (1, 0, 0), (1, 1, 0), (1, 1, 1), (0, 0, 0),
    (1, 0, 0), (1, 1, 0), (1, 1, 0), (1, 0, 0),
    (1, 0, 0), (1, 1, 0), (1, 1, 1), (1, 0, 0),
)


def pick(at, values):
    return sum(value * jnp.maximum(0, 1 - abs(at - i)) for i, value in enumerate(values) if value)


def passes(row, col, count):
    if count != 4:
        return [(partner(col, count - 1 - slot, count), 1 - min(slot, 1)) for slot in range(count - 1)]
    small = jnp.minimum(row, 2)
    at = count * (small + lax.div(small, 2) * lax.rem(row, 2)) + col
    return [(pick(at, [o[s] for o in ORDERS]), pick(at, [e[s] for e in EARLY])) for s in range(count - 1)]


def kernel(
    dims,
    species, symbol_x, symbol_y, symbol_z, table_x, table_y, table_z,
    out,
    space, mx, my, mz, sx, sy, sz, send_a, recv_a, send_b, recv_b, inverse,
    b_send, b_recv,
):
    fields, pack, rows, cols, cuts, xc, yb, zl = dims
    groups = fields // pack
    row, col = lax.axis_index("row"), lax.axis_index("col")
    chunks = chunk_list(cuts, groups)

    row_steps = list(range(rows - 1, 0, -1))
    col_steps = list(range(cols - 1, 0, -1))
    barrier = pltpu.get_barrier_semaphore()
    odd = lax.rem(row, 2)
    twin = row + 1 - 2 * odd

    batches = batch_list(len(chunks))

    def batch_of(i):
        return [i in batch for batch in batches].index(True)

    def first_part(load_sem, a_send, a_recv, ready):
        pieces = [(species.at[f], space.at[f]) for f in range(fields)]
        pieces += [(table_x.at[q], mx.at[q]) for q in range(cuts)]
        pieces += [(symbol_x, sx), (symbol_y, sy), (symbol_z, sz), (table_y, my), (table_z, mz)]
        loads = [
            None if i < pack else pltpu.make_async_copy(src, dst, load_sem.at[i])
            for i, (src, dst) in enumerate(pieces)
        ]
        loads[fields].start()
        height = space.shape[1] // PIECES
        for i in range(PIECES):
            for f in range(pack):
                part = pl.ds(i * height, height)
                pltpu.make_async_copy(species.at[f, part], space.at[f, part], load_sem.at[0]).start()
        for pair in range(rows // 2):
            @pl.when(row != 2 * pair + 1)
            def _():
                pl.semaphore_signal(barrier, inc=1, device_id={"row": 2 * pair + 1}, device_id_type=MESH)
        for step in col_steps:
            to = {"row": row - odd, "col": partner(col, step, cols)}
            pl.semaphore_signal(barrier, inc=1, device_id=to, device_id_type=MESH)

        @pl.when(odd == 1)
        def _():
            pl.semaphore_signal(barrier, inc=1, device_id={"row": twin}, device_id_type=MESH)

        for load in loads[fields + 1:fields + cuts]:
            load.start()

        for i, (g, q, n) in enumerate(chunks):
            if q == 0:
                if g == 0:
                    loads[fields].wait()
                    for load in loads[pack:fields]:
                        load.start()
                    group = space.at[pl.ds(0, pack)]
                    pltpu.make_async_copy(group, group, load_sem.at[0]).wait()
                else:
                    for k in range(pack):
                        loads[g * pack + k].wait()
                data = side_by_side(jnp.concatenate([space[g * pack + k] for k in range(pack)], axis=-1))
            if g == 0:
                for p in range(max(q, 1), q + n):
                    loads[fields + p].wait()
            for p in range(q, q + n):
                send_a[g, :, p] = left_dot(mx[p], data).reshape(rows, -1, LANES)
            if i == 0:

                @pl.when(odd == 1)
                def _():
                    pl.semaphore_wait(barrier, len(row_steps))
                    pl.semaphore_signal(ready, inc=1, device_id={"row": twin}, device_id_type=MESH)

                @pl.when(odd == 0)
                def _():
                    pl.semaphore_wait(ready, 1)

            for even_step, odd_step in zip(row_steps[1::2] + row_steps[::2], row_steps[::2] + row_steps[1::2]):
                to = partner(row, even_step, rows)
                to = to + (partner(row, odd_step, rows) - to) * odd
                pltpu.make_async_remote_copy(
                    src_ref=send_a.at[g, to, pl.ds(q, n)], dst_ref=recv_a.at[g, row, pl.ds(q, n)],
                    send_sem=a_send, recv_sem=a_recv.at[i],
                    device_id={"row": to}, device_id_type=MESH,
                ).start()
            recv_a[g, row, pl.ds(q, n)] = send_a[g, row, pl.ds(q, n)]
            if i == 0:
                for load in loads[fields + cuts:]:
                    load.start()

        for load in loads[fields + cuts:]:
            load.wait()
        part_y = jnp.zeros((yb, 1), jnp.float32)
        at = lax.broadcasted_iota(jnp.int32, (yb, 1), 0)
        for j in range(yb):
            part_y = jnp.where(at == j, sy[col * yb + j], part_y)
        for i in range(cuts * xc):
            inverse[i] = 1.0 / ((sx[row * (cuts * xc) + i] + part_y) + sz[...])


        @pl.when(odd == 0)
        def _():
            pl.semaphore_wait(barrier, 2 * len(col_steps) + 1)
            pl.semaphore_signal(ready, inc=1, device_id={"row": twin}, device_id_type=MESH)

        @pl.when(odd == 1)
        def _():
            pl.semaphore_wait(ready, 1)

        hops = passes(row, col, cols)

        def pass_on(i, slot):
            g, q, n = chunks[i]
            to = hops[slot][0]
            pltpu.make_async_remote_copy(
                src_ref=send_b.at[g, to, pl.ds(q, n)], dst_ref=recv_b.at[g, col, pl.ds(q, n)],
                send_sem=b_send, recv_sem=b_recv.at[batch_of(i)],
                device_id={"col": to}, device_id_type=MESH,
            ).start()

        for i, (g, q, n) in enumerate(chunks):
            arrived = recv_a.at[g, pl.ds(0, rows - 1), pl.ds(q, n)]
            pltpu.make_async_copy(arrived, arrived, a_recv.at[i]).wait()
            for p in range(q, q + n):
                lines = recv_a[g, :, p].reshape(-1, LANES)
                send_b[g, :, p] = left_dot(my[...], side_by_side(lines)).reshape(cols, -1, LANES)
            for slot in range(cols - 1):
                pl.when(hops[slot][1] == 1)(functools.partial(pass_on, i, slot))
            recv_b[g, col, pl.ds(q, n)] = send_b[g, col, pl.ds(q, n)]
        for slot in range(cols - 1):
            for i in range(len(chunks)):
                pl.when(hops[slot][1] == 0)(functools.partial(pass_on, i, slot))

        sent = send_a.at[:, pl.ds(0, rows - 1)]
        pltpu.make_async_copy(sent, sent, a_send).wait()

    dma = pltpu.SemaphoreType.DMA
    pl.run_scoped(first_part, dma((fields + cuts + 5,)), dma, dma((len(chunks),)), pltpu.SemaphoreType.REGULAR)

    height = xc * yb
    for batch in batches:
        lines = []
        g, q, n = chunks[batch[0]]
        arrived = recv_b.at[g, pl.ds(0, cols - 1), pl.ds(q, sum(chunks[i][2] for i in batch))]
        pltpu.make_async_copy(arrived, arrived, b_recv.at[batch_of(batch[0])]).wait()
        for i in batch:
            g, q, n = chunks[i]
            for p in range(q, q + n):
                blocks = [recv_b[g, c, p] for c in range(cols)]
                for k in range(pack):
                    lines.append(jnp.concatenate([b[:, k * zl:(k + 1) * zl] for b in blocks], axis=-1))
        high, low = split(jnp.concatenate(lines, axis=0))
        most = dot(jnp.concatenate([high, low], axis=0), mz[0])
        count = high.shape[0]
        result = most[:count] + most[count:] + dot(high, mz[1])
        at_line = 0
        for i in batch:
            g, q, n = chunks[i]
            for p in range(q, q + n):
                factor = inverse[p * xc:(p + 1) * xc].reshape(height, -1)
                for k in range(pack):
                    out[g * pack + k, pl.ds(p * height, height)] = result[at_line:at_line + height] * factor
                    at_line += height

    sent = send_b.at[:, pl.ds(0, cols - 1)]
    pltpu.make_async_copy(sent, sent, b_send).wait()


def on_device(rows, cols, species, symbol_x, symbol_y, symbol_z):
    fields, x, yl, zl = species.shape
    y, z = symbol_y.shape[0], symbol_z.shape[0]
    xb, yb = x // rows, y // cols
    pack = LANES // zl
    groups = fields // pack
    xc = max(1, SUBLANES // yl)
    cuts = xb // xc

    hx = table(x)
    eye = np.eye(yl, dtype=np.float32)
    full_x = np.einsum("rqia,yb->qriyab", hx.T.reshape(rows, cuts, xc, x), eye).reshape(cuts, rows * xc * yl, x * yl)
    hy = table(y).T.reshape(cols, yb, rows, yl)
    full_y = np.einsum("cmry,ij->cimrjy", hy, np.eye(xc, dtype=np.float32)).reshape(cols * xc * yb, rows * xc * yl)
    tables = [
        np.concatenate(list(halves(full_x)), axis=1), np.concatenate(list(halves(full_y)), axis=0), halves(table(z))
    ]

    any_space = pl.BlockSpec(memory_space=pltpu.MemorySpace.HBM)
    chunks = len(chunk_list(cuts, groups))
    a_shape = (groups, rows, cuts, xc * yl, LANES)
    b_shape = (groups, cols, cuts, xc * yb, LANES)
    dma = pltpu.SemaphoreType.DMA
    out = pl.pallas_call(
        functools.partial(kernel, (fields, pack, rows, cols, cuts, xc, yb, zl)),
        out_shape=pltpu.MemorySpace.VMEM((fields, xb * yb, z), jnp.float32),
        in_specs=[any_space] * 7,
        out_specs=pl.BlockSpec(memory_space=pltpu.MemorySpace.VMEM),
        scratch_shapes=[
            pltpu.VMEM((fields, x * yl, zl), jnp.float32),
            pltpu.VMEM(tables[0].shape, jnp.bfloat16),
            pltpu.VMEM(tables[1].shape, jnp.bfloat16),
            pltpu.VMEM(tables[2].shape, jnp.bfloat16),
            pltpu.SMEM((x,), jnp.float32),
            pltpu.SMEM((y,), jnp.float32),
            pltpu.VMEM((1, z), jnp.float32),
            pltpu.VMEM(a_shape, jnp.float32),
            pltpu.VMEM(a_shape, jnp.float32),
            pltpu.VMEM(b_shape, jnp.float32),
            pltpu.VMEM(b_shape, jnp.float32),
            pltpu.VMEM((xb, yb, z), jnp.float32),
            dma,
            dma((len(batch_list(chunks)),)),
        ],
        compiler_params=pltpu.CompilerParams(
            collective_id=0, has_side_effects=True, vmem_limit_bytes=60 * 1024 * 1024
        ),
    )(
        species.reshape(fields, x * yl, zl), symbol_x, symbol_y, symbol_z.reshape(1, z),
        *[jnp.asarray(t) for t in tables],
    )
    return out.reshape(fields, xb, yb, z)


def solution(mesh):
    placed = (P(None, None, "row", "col"), P(), P(), P())
    return jax.shard_map(
        functools.partial(on_device, mesh.shape["row"], mesh.shape["col"]),
        mesh=mesh,
        in_specs=placed,
        out_specs=P(None, "row", "col", None),
        check_vma=False,
    )
```

```python
import functools

import jax
import jax.numpy as jnp
import ml_dtypes
import numpy as np
from jax import lax
from jax.experimental import pallas as pl
from jax.experimental.pallas import tpu as pltpu
from jax.sharding import PartitionSpec as P

MESH = pl.DeviceIdType.MESH
LANES = 128
PIECES = 8
SUBLANES = 8


def table(count):
    rank = np.arange(count, dtype=np.int64) + 1
    angle = np.pi / (count + 1) * ((rank[:, None] * rank[None, :]) % (2 * count + 2))
    return (np.sin(angle) * (2.0 / (count + 1)) ** 0.5).astype(np.float32)


def halves(values):
    high = values.astype(ml_dtypes.bfloat16)
    low = (values - high.astype(np.float32)).astype(ml_dtypes.bfloat16)
    return np.stack([high, low])


def split(values):
    high = values.astype(jnp.bfloat16)
    low = (values - high.astype(jnp.float32)).astype(jnp.bfloat16)
    return high, low


def side_by_side(values):
    return jnp.concatenate(split(values), axis=-1)


def dot(a, b):
    return jnp.dot(a, b, preferred_element_type=jnp.float32)


def left_dot(both, data):
    count, width = both.shape[0] // 2, data.shape[-1] // 2
    terms = dot(both, data)
    sides = terms[:, :width] + terms[:, width:]
    return sides[:count] + sides[count:]


def partner(me, step, count):
    if count & (count - 1):
        return lax.rem(me + step, count)
    to, bit = me, 1
    while bit < count:
        if step & bit:
            to = to + bit * (1 - 2 * lax.rem(me // bit, 2))
        bit *= 2
    return to


def chunk_list(cuts, groups):
    if cuts == 4 and groups == 2:
        return [(0, 0, 1), (0, 1, 1), (0, 2, 2), (1, 0, 2), (1, 2, 2)]
    return [(g, q, 1) for g in range(groups) for q in range(cuts)]


def batch_list(count):
    return [[0, 1], [2], [3], [4]] if count == 5 else [[i] for i in range(count)]


ORDERS = (
    (3, 2, 1), (0, 3, 2), (3, 0, 1), (0, 1, 2),
    (3, 2, 1), (0, 3, 2), (3, 0, 1), (0, 1, 2),
    (3, 2, 1), (0, 3, 2), (3, 0, 1), (0, 1, 2),
    (3, 2, 1), (0, 3, 2), (3, 0, 1), (0, 2, 1),
)
EARLY = (
    (1, 0, 0), (1, 1, 0), (1, 1, 0), (1, 0, 0),
    (1, 0, 0), (1, 1, 0), (1, 1, 1), (0, 0, 0),
    (1, 0, 0), (1, 1, 0), (1, 1, 0), (1, 0, 0),
    (1, 0, 0), (1, 1, 0), (1, 1, 1), (1, 0, 0),
)


def pick(at, values):
    return sum(value * jnp.maximum(0, 1 - abs(at - i)) for i, value in enumerate(values) if value)


def passes(row, col, count):
    if count != 4:
        return [(partner(col, count - 1 - slot, count), 1 - min(slot, 1)) for slot in range(count - 1)]
    small = jnp.minimum(row, 2)
    at = count * (small + lax.div(small, 2) * lax.rem(row, 2)) + col
    return [(pick(at, [o[s] for o in ORDERS]), pick(at, [e[s] for e in EARLY])) for s in range(count - 1)]


def kernel(
    dims,
    species, symbol_x, symbol_y, symbol_z, table_x, table_y, table_z,
    out,
    space, mx, my, mz, sx, sy, sz, send_a, recv_a, send_b, recv_b, inverse,
    b_send, b_recv, ready,
):
    fields, pack, rows, cols, cuts, xc, yb, zl = dims
    groups = fields // pack
    row, col = lax.axis_index("row"), lax.axis_index("col")
    chunks = chunk_list(cuts, groups)

    row_steps = list(range(rows - 1, 0, -1))
    col_steps = list(range(cols - 1, 0, -1))
    barrier = pltpu.get_barrier_semaphore()
    odd = lax.rem(row, 2)
    twin = row + 1 - 2 * odd

    batches = batch_list(len(chunks))

    def batch_of(i):
        return [i in batch for batch in batches].index(True)

    def first_part(load_sem, a_send, a_recv):
        pieces = [(species.at[f], space.at[f]) for f in range(fields)]
        pieces += [(table_x.at[q], mx.at[q]) for q in range(cuts)]
        pieces += [(symbol_x, sx), (symbol_y, sy), (symbol_z, sz), (table_y, my), (table_z, mz)]
        loads = [
            None if i < pack else pltpu.make_async_copy(src, dst, load_sem.at[i])
            for i, (src, dst) in enumerate(pieces)
        ]
        loads[fields].start()
        height = space.shape[1] // PIECES
        for i in range(PIECES):
            for f in range(pack):
                part = pl.ds(i * height, height)
                pltpu.make_async_copy(species.at[f, part], space.at[f, part], load_sem.at[0]).start()
        for pair in range(rows // 2):
            @pl.when(row != 2 * pair + 1)
            def _():
                pl.semaphore_signal(barrier, inc=1, device_id={"row": 2 * pair + 1}, device_id_type=MESH)
        for step in col_steps:
            to = {"row": row - odd, "col": partner(col, step, cols)}
            pl.semaphore_signal(barrier, inc=1, device_id=to, device_id_type=MESH)

        @pl.when(odd == 1)
        def _():
            pl.semaphore_signal(barrier, inc=1, device_id={"row": twin}, device_id_type=MESH)

        for load in loads[fields + 1:fields + cuts]:
            load.start()

        for i, (g, q, n) in enumerate(chunks):
            if q == 0:
                if g == 0:
                    loads[fields].wait()
                    for load in loads[pack:fields]:
                        load.start()
                    group = space.at[pl.ds(0, pack)]
                    pltpu.make_async_copy(group, group, load_sem.at[0]).wait()
                else:
                    for k in range(pack):
                        loads[g * pack + k].wait()
                data = side_by_side(jnp.concatenate([space[g * pack + k] for k in range(pack)], axis=-1))
            if g == 0:
                for p in range(max(q, 1), q + n):
                    loads[fields + p].wait()
            for p in range(q, q + n):
                send_a[g, :, p] = left_dot(mx[p], data).reshape(rows, -1, LANES)
            if i == 0:

                @pl.when(odd == 1)
                def _():
                    pl.semaphore_wait(barrier, len(row_steps))
                    pl.semaphore_signal(ready, inc=1, device_id={"row": twin}, device_id_type=MESH)

                @pl.when(odd == 0)
                def _():
                    pl.semaphore_wait(ready, 1)

            for even_step, odd_step in zip(row_steps[1::2] + row_steps[::2], row_steps[::2] + row_steps[1::2]):
                to = partner(row, even_step, rows)
                to = to + (partner(row, odd_step, rows) - to) * odd
                pltpu.make_async_remote_copy(
                    src_ref=send_a.at[g, to, pl.ds(q, n)], dst_ref=recv_a.at[g, row, pl.ds(q, n)],
                    send_sem=a_send, recv_sem=a_recv.at[i],
                    device_id={"row": to}, device_id_type=MESH,
                ).start()
            recv_a[g, row, pl.ds(q, n)] = send_a[g, row, pl.ds(q, n)]
            if i == 0:
                for load in loads[fields + cuts:]:
                    load.start()

        for load in loads[fields + cuts:]:
            load.wait()
        part_y = jnp.zeros((yb, 1), jnp.float32)
        at = lax.broadcasted_iota(jnp.int32, (yb, 1), 0)
        for j in range(yb):
            part_y = jnp.where(at == j, sy[col * yb + j], part_y)
        for i in range(cuts * xc):
            inverse[i] = 1.0 / ((sx[row * (cuts * xc) + i] + part_y) + sz[...])


        @pl.when(odd == 0)
        def _():
            pl.semaphore_wait(barrier, 2 * len(col_steps) + 1)
            pl.semaphore_signal(ready, inc=1, device_id={"row": twin}, device_id_type=MESH)

        @pl.when(odd == 1)
        def _():
            pl.semaphore_wait(ready, 1)

        hops = passes(row, col, cols)

        def pass_on(i, slot):
            g, q, n = chunks[i]
            to = hops[slot][0]
            pltpu.make_async_remote_copy(
                src_ref=send_b.at[g, to, pl.ds(q, n)], dst_ref=recv_b.at[g, col, pl.ds(q, n)],
                send_sem=b_send, recv_sem=b_recv.at[batch_of(i)],
                device_id={"col": to}, device_id_type=MESH,
            ).start()

        for i, (g, q, n) in enumerate(chunks):
            arrived = recv_a.at[g, pl.ds(0, rows - 1), pl.ds(q, n)]
            pltpu.make_async_copy(arrived, arrived, a_recv.at[i]).wait()
            for p in range(q, q + n):
                lines = recv_a[g, :, p].reshape(-1, LANES)
                send_b[g, :, p] = left_dot(my[...], side_by_side(lines)).reshape(cols, -1, LANES)
            for slot in range(cols - 1):
                pl.when(hops[slot][1] == 1)(functools.partial(pass_on, i, slot))
            recv_b[g, col, pl.ds(q, n)] = send_b[g, col, pl.ds(q, n)]
        for slot in range(cols - 1):
            for i in range(len(chunks)):
                pl.when(hops[slot][1] == 0)(functools.partial(pass_on, i, slot))

        sent = send_a.at[:, pl.ds(0, rows - 1)]
        pltpu.make_async_copy(sent, sent, a_send).wait()

    dma = pltpu.SemaphoreType.DMA
    pl.run_scoped(first_part, dma((fields + cuts + 5,)), dma, dma((len(chunks),)))

    height = xc * yb
    for batch in batches:
        lines = []
        g, q, n = chunks[batch[0]]
        arrived = recv_b.at[g, pl.ds(0, cols - 1), pl.ds(q, sum(chunks[i][2] for i in batch))]
        pltpu.make_async_copy(arrived, arrived, b_recv.at[batch_of(batch[0])]).wait()
        for i in batch:
            g, q, n = chunks[i]
            for p in range(q, q + n):
                blocks = [recv_b[g, c, p] for c in range(cols)]
                for k in range(pack):
                    lines.append(jnp.concatenate([b[:, k * zl:(k + 1) * zl] for b in blocks], axis=-1))
        high, low = split(jnp.concatenate(lines, axis=0))
        most = dot(jnp.concatenate([high, low], axis=0), mz[0])
        count = high.shape[0]
        result = most[:count] + most[count:] + dot(high, mz[1])
        at_line = 0
        for i in batch:
            g, q, n = chunks[i]
            for p in range(q, q + n):
                factor = inverse[p * xc:(p + 1) * xc].reshape(height, -1)
                for k in range(pack):
                    out[g * pack + k, pl.ds(p * height, height)] = result[at_line:at_line + height] * factor
                    at_line += height

    sent = send_b.at[:, pl.ds(0, cols - 1)]
    pltpu.make_async_copy(sent, sent, b_send).wait()


def on_device(rows, cols, species, symbol_x, symbol_y, symbol_z):
    fields, x, yl, zl = species.shape
    y, z = symbol_y.shape[0], symbol_z.shape[0]
    xb, yb = x // rows, y // cols
    pack = LANES // zl
    groups = fields // pack
    xc = max(1, SUBLANES // yl)
    cuts = xb // xc

    hx = table(x)
    eye = np.eye(yl, dtype=np.float32)
    full_x = np.einsum("rqia,yb->qriyab", hx.T.reshape(rows, cuts, xc, x), eye).reshape(cuts, rows * xc * yl, x * yl)
    hy = table(y).T.reshape(cols, yb, rows, yl)
    full_y = np.einsum("cmry,ij->cimrjy", hy, np.eye(xc, dtype=np.float32)).reshape(cols * xc * yb, rows * xc * yl)
    tables = [
        np.concatenate(list(halves(full_x)), axis=1), np.concatenate(list(halves(full_y)), axis=0), halves(table(z))
    ]

    any_space = pl.BlockSpec(memory_space=pltpu.MemorySpace.HBM)
    chunks = len(chunk_list(cuts, groups))
    a_shape = (groups, rows, cuts, xc * yl, LANES)
    b_shape = (groups, cols, cuts, xc * yb, LANES)
    dma = pltpu.SemaphoreType.DMA
    out = pl.pallas_call(
        functools.partial(kernel, (fields, pack, rows, cols, cuts, xc, yb, zl)),
        out_shape=pltpu.MemorySpace.VMEM((fields, xb * yb, z), jnp.float32),
        in_specs=[any_space] * 7,
        out_specs=pl.BlockSpec(memory_space=pltpu.MemorySpace.VMEM),
        scratch_shapes=[
            pltpu.VMEM((fields, x * yl, zl), jnp.float32),
            pltpu.VMEM(tables[0].shape, jnp.bfloat16),
            pltpu.VMEM(tables[1].shape, jnp.bfloat16),
            pltpu.VMEM(tables[2].shape, jnp.bfloat16),
            pltpu.SMEM((x,), jnp.float32),
            pltpu.SMEM((y,), jnp.float32),
            pltpu.VMEM((1, z), jnp.float32),
            pltpu.VMEM(a_shape, jnp.float32),
            pltpu.VMEM(a_shape, jnp.float32),
            pltpu.VMEM(b_shape, jnp.float32),
            pltpu.VMEM(b_shape, jnp.float32),
            pltpu.VMEM((xb, yb, z), jnp.float32),
            dma,
            dma((len(batch_list(chunks)),)),
            pltpu.SemaphoreType.REGULAR,
        ],
        compiler_params=pltpu.CompilerParams(
            collective_id=0, has_side_effects=True, vmem_limit_bytes=60 * 1024 * 1024
        ),
    )(
        species.reshape(fields, x * yl, zl), symbol_x, symbol_y, symbol_z.reshape(1, z),
        *[jnp.asarray(t) for t in tables],
    )
    return out.reshape(fields, xb, yb, z)


def solution(mesh):
    placed = (P(None, None, "row", "col"), P(), P(), P())
    return jax.shard_map(
        functools.partial(on_device, mesh.shape["row"], mesh.shape["col"]),
        mesh=mesh,
        in_specs=placed,
        out_specs=P(None, "row", "col", None),
        check_vma=False,
    )
```
